256 devices in a mesh: dev: 256 (over x, y, z, core).
Axes of the slice: x: 4, y: 4, z: 8, core: 2. Of those that a mesh axis runs over, the one named last changes fastest.
Arguments:
- field: float32 [16, 16, 16, 32768], P(None, None, None, 'dev'), may hold values from -6 to 6
- s_mats: float32 [3, 18, 18], replicated, may hold values from -1.5 to 1.5
- lam: float32 [3, 18], replicated, may hold values from 0.2 to 4
- coeff: float32 [3, 32768], P(None, 'dev'), may hold values from 0.5 to 2
- nbr_src: int32 [6, 32768], P(None, 'dev'), may hold values from 0 to 7, as said below
- nbr_idx: int32 [6, 32768], P(None, 'dev'), may hold values from 0 to 767, as said below
- orient: int32 [6, 32768], P(None, 'dev'), may hold values from 0 to 3, as said below
- send_x: int32 [2, 4096], P(None, 'dev'), may hold values from 0 to 255, as said below
- send_y: int32 [2, 4096], P(None, 'dev'), may hold values from 256 to 511, as said below
- send_z: int32 [2, 16384], P(None, 'dev'), may hold values from 512 to 767, as said below
Outputs:
- smoothed: float32 [16, 16, 16, 32768], P(None, None, None, 'dev')
The draws below stay inside these ranges and needn't reach their ends.
Inputs may be any that keep to these rules, and one draw needn't show every extreme that they name: `nbr_src`: 0 where the face lies on the boundary of the box of elements, 1 where the element across it is on the same device, 2 + j where it is on the device whose index is lower by o_j. Devices form a 4 x 4 x 16 grid, first index fastest; each holds a 8 x 8 x 2 block of the box, its elements in slots in any order and each stored mirrored or not along each of its three axes. Every face not on the boundary is shared by exactly two elements and listed from both sides. `nbr_idx`: for code 1 the id g * 128 + s of the face g of the element in slot s that meets this face; for code 2 + j a position in list j of the sending device; 0 for code 0. `orient`: the two sides of a shared face carry the same code; 0 on the boundary. `send_x`: row r (list r) holds the ids of the 16 faces of this device's block on its low (r = 0) or high (r = 1) side across the first dimension, each once, ordered by the faces' block coordinates along the second dimension, then the third; the device whose index is higher by o_r reads it. Each id is that of face 0 or 1 of its element. `send_y`: as send_x, across the second dimension (lists 2 and 3), 16 faces ordered by the first block coordinate, then the third; each id is that of face 2 or 3 of its element. `send_z`: as send_x, across the third dimension (lists 4 and 5), 64 faces ordered by the first block coordinate, then the second; each id is that of face 4 or 5 of its element.
All inputs are finite; a program needn't handle non-finite values.
Results may differ from the reference program's by a relative error of at most 0.0003.
Values sent between devices are 32-bit elements; how exact they have to be, the bound alone decides.
No kernel may reach another device: no remote copies, remote signals or barrier semaphores. Data moves between devices by JAX's collectives and lax.ppermute only.
A program may use at most 128 MiB of HBM per device.

```python
import math
import jax
import jax.numpy as jnp
from jax import lax

NP = 16
NE = 18
BX = 8
BY = 8
BZ = 2
DEV_X = 4
DEV_Y = 4
ELEMS = 32768
N_DEV = 256


def block_tables(key):
    slots = BX * BY * BZ
    height = N_DEV // (DEV_X * DEV_Y)
    extents = (BX, BY, BZ)
    layout = (DEV_X, DEV_Y, height)
    device_step = (1, DEV_X, DEV_X * DEV_Y)
    place_step = (1, BX, BX * BY)
    keys = jax.random.split(jax.random.fold_in(key, 7), N_DEV)
    storage = jax.vmap(lambda part_key: jax.random.permutation(part_key, slots))(keys).astype(jnp.int32)
    placing = jnp.argsort(storage, axis=1).astype(jnp.int32)
    mirror = jax.random.randint(jax.random.fold_in(key, 8), (3, N_DEV, slots), 0, 2, dtype=jnp.int32)
    device = jnp.arange(N_DEV, dtype=jnp.int32)[:, None]
    local = (placing % BX, placing // BX % BY, placing // (BX * BY))
    owner = (device % DEV_X, device // DEV_X % DEV_Y, device // (DEV_X * DEV_Y))
    own_mirror = [jnp.take_along_axis(mirror[axis], placing, axis=1) for axis in range(3)]
    sources = []
    indices = []
    codes = []
    for face in range(6):
        axis = face // 2
        others = [other for other in range(3) if other != axis]
        side = face % 2 ^ own_mirror[axis]
        coord = owner[axis] * extents[axis] + local[axis]
        moved = coord + 2 * side - 1
        inside = (moved >= 0) & (moved < extents[axis] * layout[axis])
        moved = jnp.clip(moved, 0, extents[axis] * layout[axis] - 1)
        other_dev = device + (moved // extents[axis] - owner[axis]) * device_step[axis]
        other_place = placing + (moved % extents[axis] - local[axis]) * place_step[axis]
        flat_index = other_dev * slots + other_place
        other_slot = storage.reshape(-1)[flat_index]
        other_mirror = [mirror[other].reshape(-1)[flat_index] for other in range(3)]
        facing = 2 * axis + (1 - side ^ other_mirror[axis])
        code = (own_mirror[others[0]] ^ other_mirror[others[0]]) + 2 * (own_mirror[others[1]] ^ other_mirror[others[1]])
        same = other_dev == device
        position = local[others[0]] + extents[others[0]] * local[others[1]]
        sources.append(jnp.where(inside, jnp.where(same, 1, 2 + 2 * axis + 1 - side), 0))
        indices.append(jnp.where(inside, jnp.where(same, facing * slots + other_slot, position), 0))
        codes.append(jnp.where(inside, code, 0))
    sends = []
    for axis in range(3):
        others = [other for other in range(3) if other != axis]
        count = extents[others[0]] * extents[others[1]]
        position = jnp.arange(count, dtype=jnp.int32)
        rows = []
        for side in range(2):
            coords = [0, 0, 0]
            coords[axis] = (extents[axis] - 1) * side
            coords[others[0]] = position % extents[others[0]]
            coords[others[1]] = position // extents[others[0]]
            spot = coords[0] + BX * coords[1] + BX * BY * coords[2]
            slot = storage[:, spot]
            flip = mirror[axis][:, spot]
            face = 2 * axis + (side ^ flip)
            rows.append((face * slots + slot).reshape(-1))
        sends.append(jnp.stack(rows).astype(jnp.int32))
    shape = (6, N_DEV * slots)
    return (jnp.stack(sources).reshape(shape).astype(jnp.int32), jnp.stack(indices).reshape(shape).astype(jnp.int32), jnp.stack(codes).reshape(shape).astype(jnp.int32), sends[0], sends[1], sends[2])


def draw_nbr_src(key, part):
    return block_tables(key)[0]


def draw_nbr_idx(key, part):
    return block_tables(key)[1]


def draw_orient(key, part):
    return block_tables(key)[2]


def draw_send_x(key, part):
    return block_tables(key)[3]


def draw_send_y(key, part):
    return block_tables(key)[4]


def draw_send_z(key, part):
    return block_tables(key)[5]


def shard_levels(own_key, extent, cuts, least, top_value):
    loudness = 1.0
    for dim, parts in cuts:
        draws = jax.random.uniform(jax.random.fold_in(jax.random.fold_in(own_key, 6), dim), (parts,), jnp.float32, least / len(cuts), top_value / len(cuts))
        loudness = loudness * jnp.repeat(jnp.exp(draws), extent[dim] // parts).reshape((-1,) + (1,) * (len(extent) - 1 - dim))
    return loudness


def noise(stream_key, shape, scale, reach, shards=(), kind=jnp.bfloat16):
    drawn = jax.random.normal(stream_key, shape, jnp.float32) * scale
    if len(shards) > 0:
        drawn = shard_levels(stream_key, shape, shards, -0.22, 0.18) * drawn
    return jnp.clip(drawn, min=-reach, max=reach).astype(kind)


def setup_inputs(seed: int = 0) -> dict:
    seeds = jax.random.split(jax.random.key(seed), 11)
    return {
        "field": noise(seeds[0], (NP, NP, NP, ELEMS), 1.0, 6.0, ((3, 256),), jnp.float32),
        "s_mats": noise(seeds[1], (3, NE, NE), NE ** -0.5, 1.5, (), jnp.float32),
        "lam": jnp.clip(jnp.exp(jax.random.uniform(seeds[2], (3, NE), jnp.float32, math.log(0.2), math.log(4.0))), 0.2, 4.0),
        "coeff": jnp.clip(jnp.exp(math.log(2.0) - 1.3862944 * jax.random.uniform(seeds[3], (3, ELEMS), jnp.float32) ** shard_levels(seeds[3], (3, ELEMS), ((1, 256),), -0.2, 0.2)), 0.5, 2.0),
        "nbr_src": draw_nbr_src(jax.random.fold_in(seeds[10], 71), 0),
        "nbr_idx": draw_nbr_idx(jax.random.fold_in(seeds[10], 71), 0),
        "orient": draw_orient(jax.random.fold_in(seeds[10], 71), 0),
        "send_x": draw_send_x(jax.random.fold_in(seeds[10], 71), 0),
        "send_y": draw_send_y(jax.random.fold_in(seeds[10], 71), 0),
        "send_z": draw_send_z(jax.random.fold_in(seeds[10], 71), 0),
    }


EXACT = lax.Precision.HIGHEST


def face_planes(block):
    last = block.shape[0] - 2
    return jnp.concatenate([block[1], block[last], block[:, 1], block[:, last], block[:, :, 1], block[:, :, last]], axis=2)


def reorient(planes, codes):
    first = (codes % 2 == 1)[None, None]
    second = (codes // 2 == 1)[None, None]
    planes = jnp.where(first, jnp.flip(planes, 0), planes)
    return jnp.where(second, jnp.flip(planes, 1), planes)


def extend_box(block, ghosts):
    box = jnp.pad(block, ((1, 1), (1, 1), (1, 1), (0, 0)))
    last = box.shape[0] - 1
    box = box.at[0, 1:last, 1:last].set(ghosts[:, :, 0])
    box = box.at[last, 1:last, 1:last].set(ghosts[:, :, 1])
    box = box.at[1:last, 0, 1:last].set(ghosts[:, :, 2])
    box = box.at[1:last, last, 1:last].set(ghosts[:, :, 3])
    box = box.at[1:last, 1:last, 0].set(ghosts[:, :, 4])
    return box.at[1:last, 1:last, last].set(ghosts[:, :, 5])


def rim_layers(box):
    last = box.shape[0] - 1
    inner = slice(1, last)
    return jnp.stack([box[0, inner, inner], box[last, inner, inner], box[inner, 0, inner],
                      box[inner, last, inner], box[inner, inner, 0], box[inner, inner, last]], axis=2)


def add_layers(block, returned):
    last = block.shape[0] - 2
    block = block.at[1].add(returned[:, :, 0])
    block = block.at[last].add(returned[:, :, 1])
    block = block.at[:, 1].add(returned[:, :, 2])
    block = block.at[:, last].add(returned[:, :, 3])
    block = block.at[:, :, 1].add(returned[:, :, 4])
    return block.at[:, :, last].add(returned[:, :, 5])


def eigen_divisor(lam, scale):
    return (scale[0][None, None, None, :] * lam[0][:, None, None, None]
            + scale[1][None, None, None, :] * lam[1][None, :, None, None]
            + scale[2][None, None, None, :] * lam[2][None, None, :, None])


def solve_box(box, s_mats, divisor):
    coef = jnp.einsum('ia,ijkm->ajkm', s_mats[0], box, precision=EXACT)
    coef = jnp.einsum('jb,ajkm->abkm', s_mats[1], coef, precision=EXACT)
    coef = jnp.einsum('kc,abkm->abcm', s_mats[2], coef, precision=EXACT)
    scaled = coef / divisor
    solved = jnp.einsum('ia,abcm->ibcm', s_mats[0], scaled, precision=EXACT)
    solved = jnp.einsum('jb,ibcm->ijcm', s_mats[1], solved, precision=EXACT)
    return jnp.einsum('kc,ijcm->ijkm', s_mats[2], solved, precision=EXACT)


def reference(field, s_mats, lam, coeff, nbr_src, nbr_idx, orient, send_x, send_y, send_z):
    slots = BX * BY * BZ
    count = slots * N_DEV
    edge = field.shape[0]
    pool = jnp.concatenate([face_planes(field), jnp.zeros((edge, edge, 1), field.dtype)], axis=2)
    device = jnp.arange(count, dtype=jnp.int32) // slots
    offsets = (-1, 1, -DEV_X, DEV_X, -DEV_X * DEV_Y, DEV_X * DEV_Y)
    lists = (send_x[0], send_x[1], send_y[0], send_y[1], send_z[0], send_z[1])
    target = (nbr_idx // slots) * count + device * slots + nbr_idx % slots
    for direction in range(6):
        table = lists[direction]
        length = table.shape[0] // N_DEV
        sender = jnp.clip(device - offsets[direction], 0, N_DEV - 1)
        entry = table[jnp.clip(sender * length + nbr_idx, 0, table.shape[0] - 1)]
        remote = (entry // slots) * count + sender * slots + entry % slots
        target = jnp.where(nbr_src == 2 + direction, remote, target)
    target = jnp.where(nbr_src == 0, 6 * count, target).astype(jnp.int32)

    def one_device(number):
        start = number * slots
        block = lax.dynamic_slice_in_dim(field, start, slots, 3)
        where_from = lax.dynamic_slice_in_dim(target, start, slots, 1)
        codes = lax.dynamic_slice_in_dim(orient, start, slots, 1)
        scale = lax.dynamic_slice_in_dim(coeff, start, slots, 1)
        gathered = jnp.take(pool, where_from.reshape(-1), axis=2).reshape(edge, edge, 6, slots)
        ghosts = reorient(gathered, codes)
        solved = solve_box(extend_box(block, ghosts), s_mats, eigen_divisor(lam, scale))
        last = solved.shape[0] - 1
        return solved[1:last, 1:last, 1:last], reorient(rim_layers(solved), codes)

    inside, rims = lax.map(one_device, jnp.arange(N_DEV, dtype=jnp.int32))
    inside = jnp.moveaxis(inside, 0, 3).reshape(edge, edge, edge, count)
    values = jnp.transpose(rims, (1, 2, 3, 0, 4)).reshape(edge, edge, 6 * count)
    collected = jnp.zeros((edge, edge, 6 * count + 1), field.dtype).at[:, :, target.reshape(-1)].add(values)
    returned = collected[:, :, :6 * count].reshape(edge, edge, 6, count)
    return add_layers(inside, returned)
```

```python
import functools

import jax
import jax.numpy as jnp
from jax import lax
from jax.experimental import pallas as pl
from jax.experimental.pallas import tpu as pltpu
from jax.sharding import PartitionSpec as P

DEV_X = 4
DEV_Y = 4
OFFSETS = (-1, 1, -DEV_X, DEV_X, -DEV_X * DEV_Y, DEV_X * DEV_Y)
NP = 16
NE = 18
PLANE = NP * NP
LANES = 128
WIDE = 336
NARROW = PLANE + 4 * NP
CHUNK = 8
DEEP = NE * CHUNK
F32 = jnp.float32
BF16 = jnp.bfloat16


def neighbour_pairs(direction, size):
    axis = direction // 2
    step = 1 if direction % 2 else -1
    layout = (DEV_X, DEV_Y, size // (DEV_X * DEV_Y))
    pairs = []
    for i in range(size):
        place = (i % DEV_X, i // DEV_X % DEV_Y, i // (DEV_X * DEV_Y))
        if 0 <= place[axis] + step < layout[axis]:
            pairs.append((i, i + OFFSETS[direction]))
    return pairs


def lane_take(values, index):
    return jnp.take_along_axis(values, index, axis=1, mode="promise_in_bounds")


def lanes(shape):
    return lax.broadcasted_iota(jnp.int32, shape, 1)


def pack_axis(axis, plane, table, low_ref, high_ref):
    count = table.shape[1]
    blocks = LANES // count
    rows = PLANE // blocks
    low, high = table[0:1], table[1:2]
    forward = jnp.concatenate([low, high] * (blocks // 2), axis=1)
    backward = jnp.concatenate([high, low] * (blocks // 2), axis=1)
    patterns = []
    for ids in (forward, backward):
        ids = jnp.broadcast_to(ids, (8, LANES))
        patterns.append((ids & (LANES - 1), (ids // LANES) == 2 * axis + 1))
    lane_block = lanes((8, LANES)) // count
    for row in range(0, rows, 8):
        low_value = jnp.zeros((8, LANES), F32)
        high_value = jnp.zeros((8, LANES), F32)
        for block in range(blocks):
            slot, is_high = patterns[block % 2]
            start = block * rows + row
            got = jnp.where(is_high, lane_take(plane(1, start), slot), lane_take(plane(0, start), slot))
            low_value = jnp.where(lane_block == block, got, low_value)
            high_value = jnp.where(lane_block == block ^ 1, got, high_value)
        low_ref[row : row + 8] = low_value
        high_ref[row : row + 8] = high_value


def unpack_face(face, plane, low_ref, high_ref, source, index, code, put):
    axis = face // 2
    rows = low_ref.shape[0]
    blocks = PLANE // rows
    count = LANES // blocks
    full = lambda row: jnp.broadcast_to(row, (8, LANES))
    source, index, code = full(source), full(index), full(code)
    slot = index & (LANES - 1)
    local_high = (source == 1) & ((index // LANES) == 2 * axis + 1)
    local = source == 1
    from_low = source == 2 + 2 * axis
    from_high = source == 3 + 2 * axis
    position = index & (count - 1)
    flip_first = (code & 1) == 1
    flip_second = (code & 2) == 2
    reverse = 7 - lax.broadcasted_iota(jnp.int32, (8, LANES), 0)

    def fetch(start):
        block, row = start // rows, start % rows
        here = jnp.where(local_high, lane_take(plane(1, start), slot), lane_take(plane(0, start), slot))
        low = lane_take(low_ref[row : row + 8], position + block * count)
        high = lane_take(high_ref[row : row + 8], position + (block ^ 1) * count)
        away = jnp.where(from_low, low, jnp.where(from_high, high, 0.0))
        return jnp.where(local, here, away)

    def turn(value):
        return jnp.take_along_axis(value, reverse, axis=0, mode="promise_in_bounds")

    for p in range(NP // 2):
        q = NP - 1 - p
        pieces = [[fetch(line * NP), fetch(line * NP + 8)] for line in (p, q)]
        for line, near, far in ((p, pieces[0], pieces[1]), (q, pieces[1], pieces[0])):
            first = [jnp.where(flip_first, far[h], near[h]) for h in range(2)]
            put(line, [jnp.where(flip_second, turn(first[1 - h]), first[h]) for h in range(2)])


def field_plane(field_ref, axis):
    def plane(side, start):
        layer = 1 if side == 0 else NP - 2
        if axis == 0:
            return field_ref[layer * PLANE + start : layer * PLANE + start + 8]
        if axis == 1:
            base = (start // NP) * PLANE + layer * NP + start % NP
            return field_ref[base : base + 8]
        return field_ref[pl.ds(start * NP + layer, 8, stride=NP)]

    return plane


def rim_plane(rim_ref, axis):
    def plane(side, start):
        base = (2 * axis + side) * PLANE + start
        return rim_ref[base : base + 8]

    return plane


def pack_kernel(field_ref, sx_ref, sy_ref, sz_ref, *out_refs):
    for axis, table_ref in enumerate((sx_ref, sy_ref, sz_ref)):
        pack_axis(axis, field_plane(field_ref, axis), table_ref[...], out_refs[2 * axis], out_refs[2 * axis + 1])


def split(value):
    high = value.astype(BF16)
    return high, (value - high.astype(F32)).astype(BF16)


def stacked(value):
    high, low = split(value)
    return jnp.concatenate([high, high, low], axis=0)


def operator(value):
    high, low = split(value)
    return jnp.concatenate([high, low, high], axis=1)


def exact_dot(a, b):
    return jnp.dot(a, b, precision=lax.Precision.HIGHEST, preferred_element_type=F32)


def operators_kernel(s_ref, lam_ref, coeff_ref, main_ref, rim_ref, back_ref, to_ref, from_ref, base_ref):
    iota = lambda shape, dim: lax.broadcasted_iota(jnp.int32, shape, dim)

    def node(kidx, small_first):
        inner = kidx < PLANE
        t = kidx - PLANE
        group = t // NP
        along = 1 + t % NP
        if small_first:
            return jnp.where(inner, 1 + kidx // NP, jnp.where(group == 0, 0, jnp.where(group == 1, NE - 1, along)))
        return jnp.where(inner, 1 + kidx % NP, jnp.where(group == 2, 0, jnp.where(group == 3, NE - 1, along)))

    def hot(cond):
        return jnp.where(cond, 1.0, 0.0).astype(F32)

    wide_b = hot(iota((WIDE, NE), 0) // NE == iota((WIDE, NE), 1))
    wide_c = hot((iota((WIDE, NE), 0) % NE == iota((WIDE, NE), 1)) & (iota((WIDE, NE), 0) < NE * NE))
    wide_bt = hot(iota((NE, WIDE), 1) // NE == iota((NE, WIDE), 0))
    wide_ct = hot((iota((NE, WIDE), 1) % NE == iota((NE, WIDE), 0)) & (iota((NE, WIDE), 1) < NE * NE))
    node_j = hot(node(iota((NARROW, NE), 0), True) == iota((NARROW, NE), 1))
    node_k = hot(node(iota((NARROW, NE), 0), False) == iota((NARROW, NE), 1))
    node_jt = hot(node(iota((NE, NARROW), 1), True) == iota((NE, NARROW), 0))
    node_kt = hot(node(iota((NE, NARROW), 1), False) == iota((NE, NARROW), 0))
    s0, s1, s2 = s_ref[0], s_ref[1], s_ref[2]
    t0, t1, t2 = s0.T, s1.T, s2.T
    ahead = exact_dot(wide_b, exact_dot(t1, node_jt)) * exact_dot(wide_c, exact_dot(t2, node_kt))
    main_ref[...] = operator(ahead[:, :PLANE])
    rim_ref[...] = operator(ahead[:, PLANE:])
    back = exact_dot(node_j, exact_dot(s1, wide_bt)) * exact_dot(node_k, exact_dot(s2, wide_ct))
    back_ref[...] = operator(back)
    deep = hot(iota((DEEP, NE), 0) // CHUNK == iota((DEEP, NE), 1))
    deep_t = hot(iota((NE, DEEP), 1) // CHUNK == iota((NE, DEEP), 0))
    same = hot(iota((DEEP, DEEP), 0) % CHUNK == iota((DEEP, DEEP), 1) % CHUNK)
    to_ref[...] = operator(exact_dot(deep, exact_dot(t0, deep_t)) * same)
    from_ref[...] = operator(exact_dot(deep, exact_dot(s0, deep_t)) * same)
    col_b = jnp.sum(wide_b * lam_ref[1:2], axis=1, keepdims=True)
    col_c = jnp.sum(wide_c * lam_ref[2:3], axis=1, keepdims=True)
    base_ref[...] = col_b * coeff_ref[1:2] + col_c * coeff_ref[2:3]


def mm(a, b):
    return jnp.dot(a, b, preferred_element_type=F32)


def solve_kernel(
    field_ref, src_ref, idx_ref, code_ref, sx_ref, sy_ref, sz_ref, lam_ref, coeff_ref,
    main_ref, rim_op_ref, back_ref, to_ref, from_ref, base_ref,
    m0, m1, m2, m3, m4, m5,
    inner_ref, rim_ref, o0, o1, o2, o3, o4, o5,
    ghost_ref, work_ref,
):
    messages = (m0, m1, m2, m3, m4, m5)
    outs = (o0, o1, o2, o3, o4, o5)
    for face in range(6):
        axis = face // 2

        def put(line, pieces, face=face):
            for h in range(2):
                ghost_ref[pl.ds(face * PLANE + line * NP + 8 * h, 8)] = pieces[h]

        unpack_face(
            face, field_plane(field_ref, axis), messages[2 * axis], messages[2 * axis + 1],
            src_ref[face : face + 1], idx_ref[face : face + 1], code_ref[face : face + 1], put,
        )

    both = lambda load: jnp.concatenate([load(0), load(1)], axis=1)
    for pair in range(NP // 2):
        i = lambda s: 2 * pair + s
        inside = both(lambda s: field_ref[i(s) * PLANE : (i(s) + 1) * PLANE])
        edge = jnp.concatenate(
            [both(lambda s: ghost_ref[f * PLANE + i(s) * NP : f * PLANE + (i(s) + 1) * NP]) for f in range(2, 6)], axis=0
        )
        got = mm(main_ref[...], stacked(inside)) + mm(rim_op_ref[...], stacked(edge))
        for s in range(2):
            work_ref[1 + i(s)] = got[:, s * LANES : (s + 1) * LANES]
    got = mm(main_ref[...], stacked(both(lambda s: ghost_ref[s * PLANE : (s + 1) * PLANE])))
    work_ref[0] = got[:, :LANES]
    work_ref[NE - 1] = got[:, LANES:]

    scale = coeff_ref[0:1]

    def middle(step):
        rows = [pl.ds(pl.multiple_of((2 * step + s) * CHUNK, CHUNK), CHUNK) for s in range(2)]
        chunk = both(lambda s: work_ref[:, rows[s], :].reshape(DEEP, LANES))
        coef = mm(to_ref[...], stacked(chunk))
        divisor = both(
            lambda s: jnp.concatenate([lam_ref[0, a] * scale + base_ref[rows[s], :] for a in range(NE)], axis=0)
        )
        solved = mm(from_ref[...], stacked(coef / divisor))
        for s in range(2):
            work_ref[:, rows[s], :] = solved[:, s * LANES : (s + 1) * LANES].reshape(NE, CHUNK, LANES)

    for step in range(WIDE // CHUNK // 2):
        middle(step)

    got = mm(back_ref[:PLANE], stacked(both(lambda s: work_ref[s * (NE - 1)])))
    rim_ref[0:PLANE] = got[:, :LANES]
    rim_ref[PLANE : 2 * PLANE] = got[:, LANES:]
    for pair in range(NP // 2):
        got = mm(back_ref[...], stacked(both(lambda s: work_ref[1 + 2 * pair + s])))
        for s in range(2):
            i = 2 * pair + s
            part = got[:, s * LANES : (s + 1) * LANES]
            inner_ref[i * PLANE : (i + 1) * PLANE] = part[:PLANE]
            for f in range(2, 6):
                start = PLANE + (f - 2) * NP
                rim_ref[f * PLANE + i * NP : f * PLANE + (i + 1) * NP] = part[start : start + NP]
    for axis, table_ref in enumerate((sx_ref, sy_ref, sz_ref)):
        pack_axis(axis, rim_plane(rim_ref, axis), table_ref[...], outs[2 * axis], outs[2 * axis + 1])


def finish_kernel(inner_ref, rim_ref, src_ref, idx_ref, code_ref, m0, m1, m2, m3, m4, m5, out_ref):
    messages = (m0, m1, m2, m3, m4, m5)
    out_ref[...] = inner_ref[...]
    for face in range(6):
        axis = face // 2
        layer = 1 if face % 2 == 0 else NP - 2

        def put(line, pieces, axis=axis, layer=layer):
            for h in range(2):
                if axis == 0:
                    place = pl.ds(layer * PLANE + line * NP + 8 * h, 8)
                elif axis == 1:
                    place = pl.ds(line * PLANE + layer * NP + 8 * h, 8)
                else:
                    place = pl.ds((line * NP + 8 * h) * NP + layer, 8, stride=NP)
                out_ref[place] = out_ref[place] + pieces[h]

        unpack_face(
            face, rim_plane(rim_ref, axis), messages[2 * axis], messages[2 * axis + 1],
            src_ref[face : face + 1], idx_ref[face : face + 1], code_ref[face : face + 1], put,
        )


VMEM = pl.BlockSpec(memory_space=pltpu.VMEM)
SMEM = pl.BlockSpec(memory_space=pltpu.SMEM)


def message_shapes(tables):
    shapes = []
    for table in tables:
        rows = PLANE * table.shape[1] // LANES
        shapes += [jax.ShapeDtypeStruct((rows, LANES), F32)] * 2
    return shapes


def exchange(messages):
    arrived = []
    for direction in range(6):
        pairs = neighbour_pairs(direction, lax.axis_size("dev"))
        arrived.append(lax.ppermute(messages[direction], "dev", pairs))
    return arrived


def shards(field, s_mats, lam, coeff, nbr_src, nbr_idx, orient, send_x, send_y, send_z):
    flat = field.reshape(NP * PLANE, LANES)
    tables = (send_x, send_y, send_z)
    shape = jax.ShapeDtypeStruct
    outgoing = pl.pallas_call(
        pack_kernel, out_shape=message_shapes(tables), in_specs=[VMEM] * 4, out_specs=[VMEM] * 6, name="pack",
    )(flat, *tables)
    arrived = exchange(outgoing)
    operators = pl.pallas_call(
        operators_kernel,
        out_shape=[
            shape((WIDE, 3 * PLANE), BF16), shape((WIDE, 12 * NP), BF16), shape((NARROW, 3 * WIDE), BF16),
            shape((DEEP, 3 * DEEP), BF16), shape((DEEP, 3 * DEEP), BF16), shape((WIDE, LANES), F32),
        ],
        in_specs=[VMEM] * 3, out_specs=[VMEM] * 6, name="operators",
    )(s_mats, lam, coeff)
    solved = pl.pallas_call(
        solve_kernel,
        out_shape=[shape((NP * PLANE, LANES), F32), shape((6 * PLANE, LANES), F32)] + message_shapes(tables),
        in_specs=[VMEM] * 7 + [SMEM] + [VMEM] * 13, out_specs=[VMEM] * 8,
        scratch_shapes=[pltpu.VMEM((6 * PLANE, LANES), F32), pltpu.VMEM((NE, WIDE, LANES), F32)],
        name="solve",
    )(flat, nbr_src, nbr_idx, orient, *tables, lam, coeff, *operators, *arrived)
    inner, rims = solved[:2]
    returned = exchange(solved[2:])
    out = pl.pallas_call(
        finish_kernel, out_shape=shape((NP * PLANE, LANES), F32), in_specs=[VMEM] * 11, out_specs=VMEM, name="finish",
    )(inner, rims, nbr_src, nbr_idx, orient, *returned)
    return out.reshape(field.shape)


def solution(mesh):
    split_last = P(None, "dev")
    placed = (P(None, None, None, "dev"), P(), P()) + (split_last,) * 7
    return jax.shard_map(
        shards, mesh=mesh, in_specs=placed, out_specs=P(None, None, None, "dev"), check_vma=False
    )
```

```python
import jax
import jax.numpy as jnp
from jax import lax
from jax.experimental import pallas as pl
from jax.experimental.pallas import tpu as pltpu
from jax.sharding import PartitionSpec as P


DEV_X = 4
DEV_Y = 4
ORDER = (5, 0, 3, 1, 4, 2)
NP = 16
NE = 18
PLANE = NP * NP
LANES = 128
WIDE = 336
NARROW = PLANE + 4 * NP
CHUNK = 8
DEEP = NE * CHUNK
F32 = jnp.float32
BF16 = jnp.bfloat16


def swap_pairs(axis, turn, size):
    layout = (DEV_X, DEV_Y, size // (DEV_X * DEV_Y))
    stride = (1, DEV_X, DEV_X * DEV_Y)[axis]
    pairs = []
    for i in range(size):
        place = i // stride % layout[axis]
        other = place + 1 if place % 2 == turn else place - 1
        if 0 <= other < layout[axis]:
            pairs.append((i, i + (other - place) * stride))
        else:
            pairs.append((i, i ^ (DEV_X - 1 if axis == 0 else 1)))
    return pairs


def odd_place(axis):
    stride = (1, DEV_X, DEV_X * DEV_Y)[axis]
    return (lax.axis_index("dev") // stride) % 2 == 1


def lane_take(values, index):
    return jnp.take_along_axis(values, index, axis=1, mode="promise_in_bounds")


def lanes(shape):
    return lax.broadcasted_iota(jnp.int32, shape, 1)


def pack_axis(axis, plane, table, odd, first_ref, second_ref):
    count = table.shape[1]
    blocks = LANES // count
    rows = PLANE // blocks
    first = jnp.where(odd, table[0:1], table[1:2])
    second = jnp.where(odd, table[1:2], table[0:1])
    forward = jnp.concatenate([first, second] * (blocks // 2), axis=1)
    backward = jnp.concatenate([second, first] * (blocks // 2), axis=1)
    patterns = []
    for ids in (forward, backward):
        ids = jnp.broadcast_to(ids, (8, LANES))
        patterns.append((ids & (LANES - 1), (ids // LANES) == 2 * axis + 1))
    lane_block = lanes((8, LANES)) // count
    for row in range(0, rows, 8):
        first_value = jnp.zeros((8, LANES), F32)
        second_value = jnp.zeros((8, LANES), F32)
        for block in range(blocks):
            slot, is_high = patterns[block % 2]
            start = block * rows + row
            got = jnp.where(is_high, lane_take(plane(1, start), slot), lane_take(plane(0, start), slot))
            first_value = jnp.where(lane_block == block, got, first_value)
            second_value = jnp.where(lane_block == block ^ 1, got, second_value)
        first_ref[row : row + 8] = first_value
        second_ref[row : row + 8] = second_value


def unpack_face(face, plane, odd, first_ref, second_ref, source, index, code, put):
    axis = face // 2
    rows = first_ref.shape[0]
    blocks = PLANE // rows
    count = LANES // blocks
    full = lambda row: jnp.broadcast_to(row, (8, LANES))
    source, index, code = full(source), full(index), full(code)
    slot = index & (LANES - 1)
    local_high = (source == 1) & ((index // LANES) == 2 * axis + 1)
    local = source == 1
    from_first = source == jnp.where(odd, 3 + 2 * axis, 2 + 2 * axis)
    from_second = source == jnp.where(odd, 2 + 2 * axis, 3 + 2 * axis)
    position = index & (count - 1)
    flip_first = (code & 1) == 1
    flip_second = (code & 2) == 2
    reverse = 7 - lax.broadcasted_iota(jnp.int32, (8, LANES), 0)

    def fetch(start):
        block, row = start // rows, start % rows
        here = jnp.where(local_high, lane_take(plane(1, start), slot), lane_take(plane(0, start), slot))
        one = lane_take(first_ref[row : row + 8], position + block * count)
        two = lane_take(second_ref[row : row + 8], position + (block ^ 1) * count)
        away = jnp.where(from_first, one, jnp.where(from_second, two, 0.0))
        return jnp.where(local, here, away)

    def turn(value):
        return jnp.take_along_axis(value, reverse, axis=0, mode="promise_in_bounds")

    for p in range(NP // 2):
        q = NP - 1 - p
        pieces = [[fetch(line * NP), fetch(line * NP + 8)] for line in (p, q)]
        for line, near, far in ((p, pieces[0], pieces[1]), (q, pieces[1], pieces[0])):
            first = [jnp.where(flip_first, far[h], near[h]) for h in range(2)]
            put(line, [jnp.where(flip_second, turn(first[1 - h]), first[h]) for h in range(2)])


def field_plane(field_ref, axis):
    def plane(side, start):
        layer = 1 if side == 0 else NP - 2
        if axis == 0:
            return field_ref[layer * PLANE + start : layer * PLANE + start + 8]
        if axis == 1:
            base = (start // NP) * PLANE + layer * NP + start % NP
            return field_ref[base : base + 8]
        return field_ref[pl.ds(start * NP + layer, 8, stride=NP)]

    return plane


def rim_plane(rim_ref, axis):
    def plane(side, start):
        base = (2 * axis + side) * PLANE + start
        return rim_ref[base : base + 8]

    return plane


def pack_kernel(field_ref, sx_ref, sy_ref, sz_ref, *out_refs):
    for axis, table_ref in enumerate((sx_ref, sy_ref, sz_ref)):
        pack_axis(axis, field_plane(field_ref, axis), table_ref[...], odd_place(axis), out_refs[2 * axis], out_refs[2 * axis + 1])


def split(value):
    high = value.astype(BF16)
    return high, (value - high.astype(F32)).astype(BF16)


def stacked(value):
    high, low = split(value)
    return jnp.concatenate([high, high, low], axis=0)


def operator(value):
    high, low = split(value)
    return jnp.concatenate([high, low, high], axis=1)


def exact_dot(a, b):
    return jnp.dot(a, b, precision=lax.Precision.HIGHEST, preferred_element_type=F32)


def operators_kernel(s_ref, lam_ref, coeff_ref, main_ref, rim_ref, back_ref, to_ref, from_ref, base_ref):
    iota = lambda shape, dim: lax.broadcasted_iota(jnp.int32, shape, dim)

    def node(kidx, small_first):
        inner = kidx < PLANE
        t = kidx - PLANE
        group = t // NP
        along = 1 + t % NP
        if small_first:
            return jnp.where(inner, 1 + kidx // NP, jnp.where(group == 0, 0, jnp.where(group == 1, NE - 1, along)))
        return jnp.where(inner, 1 + kidx % NP, jnp.where(group == 2, 0, jnp.where(group == 3, NE - 1, along)))

    def hot(cond):
        return jnp.where(cond, 1.0, 0.0).astype(F32)

    wide_b = hot(iota((WIDE, NE), 0) // NE == iota((WIDE, NE), 1))
    wide_c = hot((iota((WIDE, NE), 0) % NE == iota((WIDE, NE), 1)) & (iota((WIDE, NE), 0) < NE * NE))
    wide_bt = hot(iota((NE, WIDE), 1) // NE == iota((NE, WIDE), 0))
    wide_ct = hot((iota((NE, WIDE), 1) % NE == iota((NE, WIDE), 0)) & (iota((NE, WIDE), 1) < NE * NE))
    node_j = hot(node(iota((NARROW, NE), 0), True) == iota((NARROW, NE), 1))
    node_k = hot(node(iota((NARROW, NE), 0), False) == iota((NARROW, NE), 1))
    node_jt = hot(node(iota((NE, NARROW), 1), True) == iota((NE, NARROW), 0))
    node_kt = hot(node(iota((NE, NARROW), 1), False) == iota((NE, NARROW), 0))
    s0, s1, s2 = s_ref[0], s_ref[1], s_ref[2]
    t0, t1, t2 = s0.T, s1.T, s2.T
    ahead = exact_dot(wide_b, exact_dot(t1, node_jt)) * exact_dot(wide_c, exact_dot(t2, node_kt))
    main_ref[...] = operator(ahead[:, :PLANE])
    rim_ref[...] = operator(ahead[:, PLANE:])
    back = exact_dot(node_j, exact_dot(s1, wide_bt)) * exact_dot(node_k, exact_dot(s2, wide_ct))
    back_ref[...] = operator(back)
    deep = hot(iota((DEEP, NE), 0) // CHUNK == iota((DEEP, NE), 1))
    deep_t = hot(iota((NE, DEEP), 1) // CHUNK == iota((NE, DEEP), 0))
    same = hot(iota((DEEP, DEEP), 0) % CHUNK == iota((DEEP, DEEP), 1) % CHUNK)
    to_ref[...] = operator(exact_dot(deep, exact_dot(t0, deep_t)) * same)
    from_ref[...] = operator(exact_dot(deep, exact_dot(s0, deep_t)) * same)
    col_b = jnp.sum(wide_b * lam_ref[1:2], axis=1, keepdims=True)
    col_c = jnp.sum(wide_c * lam_ref[2:3], axis=1, keepdims=True)
    base_ref[...] = col_b * coeff_ref[1:2] + col_c * coeff_ref[2:3]


def mm(a, b):
    return jnp.dot(a, b, preferred_element_type=F32)


def solve_kernel(
    field_ref, src_ref, idx_ref, code_ref, sx_ref, sy_ref, sz_ref, lam_ref, coeff_ref,
    main_ref, rim_op_ref, back_ref, to_ref, from_ref, base_ref,
    m0, m1, m2, m3, m4, m5,
    inner_ref, rim_ref, o0, o1, o2, o3, o4, o5,
    ghost_ref, work_ref,
):
    messages = (m0, m1, m2, m3, m4, m5)
    outs = (o0, o1, o2, o3, o4, o5)
    for face in range(6):
        axis = face // 2

        def put(line, pieces, face=face):
            for h in range(2):
                ghost_ref[pl.ds(face * PLANE + line * NP + 8 * h, 8)] = pieces[h]

        unpack_face(
            face, field_plane(field_ref, axis), odd_place(axis), messages[2 * axis], messages[2 * axis + 1],
            src_ref[face : face + 1], idx_ref[face : face + 1], code_ref[face : face + 1], put,
        )

    both = lambda load: jnp.concatenate([load(0), load(1)], axis=1)
    for pair in range(NP // 2):
        i = lambda s: 2 * pair + s
        inside = both(lambda s: field_ref[i(s) * PLANE : (i(s) + 1) * PLANE])
        edge = jnp.concatenate(
            [both(lambda s: ghost_ref[f * PLANE + i(s) * NP : f * PLANE + (i(s) + 1) * NP]) for f in range(2, 6)], axis=0
        )
        got = mm(main_ref[...], stacked(inside)) + mm(rim_op_ref[...], stacked(edge))
        for s in range(2):
            work_ref[1 + i(s)] = got[:, s * LANES : (s + 1) * LANES]
    got = mm(main_ref[...], stacked(both(lambda s: ghost_ref[s * PLANE : (s + 1) * PLANE])))
    work_ref[0] = got[:, :LANES]
    work_ref[NE - 1] = got[:, LANES:]

    scale = coeff_ref[0:1]

    def middle(step):
        rows = [pl.ds(pl.multiple_of((2 * step + s) * CHUNK, CHUNK), CHUNK) for s in range(2)]
        chunk = both(lambda s: work_ref[:, rows[s], :].reshape(DEEP, LANES))
        coef = mm(to_ref[...], stacked(chunk))
        divisor = both(
            lambda s: jnp.concatenate([lam_ref[0, a] * scale + base_ref[rows[s], :] for a in range(NE)], axis=0)
        )
        solved = mm(from_ref[...], stacked(coef / divisor))
        for s in range(2):
            work_ref[:, rows[s], :] = solved[:, s * LANES : (s + 1) * LANES].reshape(NE, CHUNK, LANES)

    for step in range(WIDE // CHUNK // 2):
        middle(step)

    got = mm(back_ref[:PLANE], stacked(both(lambda s: work_ref[s * (NE - 1)])))
    rim_ref[0:PLANE] = got[:, :LANES]
    rim_ref[PLANE : 2 * PLANE] = got[:, LANES:]
    for pair in range(NP // 2):
        got = mm(back_ref[...], stacked(both(lambda s: work_ref[1 + 2 * pair + s])))
        for s in range(2):
            i = 2 * pair + s
            part = got[:, s * LANES : (s + 1) * LANES]
            inner_ref[i * PLANE : (i + 1) * PLANE] = part[:PLANE]
            for f in range(2, 6):
                start = PLANE + (f - 2) * NP
                rim_ref[f * PLANE + i * NP : f * PLANE + (i + 1) * NP] = part[start : start + NP]
    for axis, table_ref in enumerate((sx_ref, sy_ref, sz_ref)):
        pack_axis(axis, rim_plane(rim_ref, axis), table_ref[...], odd_place(axis), outs[2 * axis], outs[2 * axis + 1])


def finish_kernel(inner_ref, rim_ref, src_ref, idx_ref, code_ref, m0, m1, m2, m3, m4, m5, out_ref):
    messages = (m0, m1, m2, m3, m4, m5)
    out_ref[...] = inner_ref[...]
    for face in range(6):
        axis = face // 2
        layer = 1 if face % 2 == 0 else NP - 2

        def put(line, pieces, axis=axis, layer=layer):
            for h in range(2):
                if axis == 0:
                    place = pl.ds(layer * PLANE + line * NP + 8 * h, 8)
                elif axis == 1:
                    place = pl.ds(line * PLANE + layer * NP + 8 * h, 8)
                else:
                    place = pl.ds((line * NP + 8 * h) * NP + layer, 8, stride=NP)
                out_ref[place] = out_ref[place] + pieces[h]

        unpack_face(
            face, rim_plane(rim_ref, axis), odd_place(axis), messages[2 * axis], messages[2 * axis + 1],
            src_ref[face : face + 1], idx_ref[face : face + 1], code_ref[face : face + 1], put,
        )


VMEM = pl.BlockSpec(memory_space=pltpu.VMEM)
SMEM = pl.BlockSpec(memory_space=pltpu.SMEM)


def grant(mebibytes):
    return pltpu.CompilerParams(vmem_limit_bytes=mebibytes << 20)


def message_shapes(tables):
    shapes = []
    for table in tables:
        rows = PLANE * table.shape[1] // LANES
        shapes += [jax.ShapeDtypeStruct((rows, LANES), F32)] * 2
    return shapes


def exchange(messages):
    arrived = [None] * 6
    for number in ORDER:
        pairs = swap_pairs(number // 2, number % 2, lax.axis_size("dev"))
        arrived[number] = lax.ppermute(messages[number], "dev", pairs)
    return arrived


def shards(field, s_mats, lam, coeff, nbr_src, nbr_idx, orient, send_x, send_y, send_z):
    flat = field.reshape(NP * PLANE, LANES)
    tables = (send_x, send_y, send_z)
    shape = jax.ShapeDtypeStruct
    outgoing = pl.pallas_call(
        pack_kernel, out_shape=message_shapes(tables), in_specs=[VMEM] * 4, out_specs=[VMEM] * 6, name="pack",
        compiler_params=grant(8),
    )(flat, *tables)
    arrived = exchange(outgoing)
    operators = pl.pallas_call(
        operators_kernel,
        out_shape=[
            shape((WIDE, 3 * PLANE), BF16), shape((WIDE, 12 * NP), BF16), shape((NARROW, 3 * WIDE), BF16),
            shape((DEEP, 3 * DEEP), BF16), shape((DEEP, 3 * DEEP), BF16), shape((WIDE, LANES), F32),
        ],
        in_specs=[VMEM] * 3, out_specs=[VMEM] * 6, name="operators",
        compiler_params=grant(16),
    )(s_mats, lam, coeff)
    solved = pl.pallas_call(
        solve_kernel,
        out_shape=[shape((NP * PLANE, LANES), F32), shape((6 * PLANE, LANES), F32)] + message_shapes(tables),
        in_specs=[VMEM] * 7 + [SMEM] + [VMEM] * 13, out_specs=[VMEM] * 8,
        scratch_shapes=[pltpu.VMEM((6 * PLANE, LANES), F32), pltpu.VMEM((NE, WIDE, LANES), F32)],
        name="solve", compiler_params=grant(24),
    )(flat, nbr_src, nbr_idx, orient, *tables, lam, coeff, *operators, *arrived)
    inner, rims = solved[:2]
    returned = exchange(solved[2:])
    out = pl.pallas_call(
        finish_kernel, out_shape=shape((NP * PLANE, LANES), F32), in_specs=[VMEM] * 11, out_specs=VMEM, name="finish",
        compiler_params=grant(12),
    )(inner, rims, nbr_src, nbr_idx, orient, *returned)
    return out.reshape(field.shape)


def solution(mesh):
    split_last = P(None, "dev")
    placed = (P(None, None, None, "dev"), P(), P()) + (split_last,) * 7
    return jax.shard_map(shards, mesh=mesh, in_specs=placed, out_specs=P(None, None, None, "dev"), check_vma=False)
```

```python
import jax
import jax.numpy as jnp
from jax import lax
from jax.experimental import pallas as pl
from jax.experimental.pallas import tpu as pltpu
from jax.sharding import PartitionSpec as P


DEV_X = 4
DEV_Y = 4
ORDERS = ((5, 4, 0, 1, 2, 3), (5, 4, 0, 1, 2, 3))
NP = 16
NE = 18
PLANE = NP * NP
LANES = 128
WIDE = 336
NARROW = PLANE + 4 * NP
CHUNK = 8
DEEP = NE * CHUNK
F32 = jnp.float32
BF16 = jnp.bfloat16


def swap_pairs(axis, turn, size):
    layout = (DEV_X, DEV_Y, size // (DEV_X * DEV_Y))
    stride = (1, DEV_X, DEV_X * DEV_Y)[axis]
    pairs = []
    for i in range(size):
        place = i // stride % layout[axis]
        other = place + 1 if place % 2 == turn else place - 1
        if 0 <= other < layout[axis]:
            pairs.append((i, i + (other - place) * stride))
        else:
            pairs.append((i, i ^ (DEV_X - 1 if axis == 0 else 1)))
    return pairs


def odd_place(axis):
    stride = (1, DEV_X, DEV_X * DEV_Y)[axis]
    return (lax.axis_index("dev") // stride) % 2 == 1


def lane_take(values, index):
    return jnp.take_along_axis(values, index, axis=1, mode="promise_in_bounds")


def lanes(shape):
    return lax.broadcasted_iota(jnp.int32, shape, 1)


def block_ids(table, odd):
    first = jnp.where(odd, table[0:1], table[1:2])
    second = jnp.where(odd, table[1:2], table[0:1])
    repeats = LANES // table.shape[1] // 2
    return [jnp.concatenate(pair * repeats, axis=1) for pair in ([first, second], [second, first])]


def pack_axis(axis, plane, ids, count, first_ref, second_ref):
    blocks = LANES // count
    rows = PLANE // blocks
    patterns = []
    for row in ids:
        row = jnp.broadcast_to(row, (8, LANES))
        patterns.append((row & (LANES - 1), (row // LANES) == 2 * axis + 1))
    lane_block = lanes((8, LANES)) // count
    for row in range(0, rows, 8):
        first_value = jnp.zeros((8, LANES), F32)
        second_value = jnp.zeros((8, LANES), F32)
        for block in range(blocks):
            slot, is_high = patterns[block % 2]
            start = block * rows + row
            got = jnp.where(is_high, lane_take(plane(1, start), slot), lane_take(plane(0, start), slot))
            first_value = jnp.where(lane_block == block, got, first_value)
            second_value = jnp.where(lane_block == block ^ 1, got, second_value)
        first_ref[row : row + 8] = first_value
        second_ref[row : row + 8] = second_value


def local_face(face, plane, source, index, put):
    axis = face // 2
    full = lambda row: jnp.broadcast_to(row, (8, LANES))
    source, index = full(source), full(index)
    slot = index & (LANES - 1)
    local = source == 1
    high = (index // LANES) == 2 * axis + 1
    for start in range(0, PLANE, 8):
        here = jnp.where(high, lane_take(plane(1, start), slot), lane_take(plane(0, start), slot))
        put(start, jnp.where(local, here, 0.0))


def unpack_face(face, local, odd, first_ref, second_ref, source, index, code):
    axis = face // 2
    rows = first_ref.shape[0]
    blocks = PLANE // rows
    count = LANES // blocks
    full = lambda row: jnp.broadcast_to(row, (8, LANES))
    source, index, code = full(source), full(index), full(code)
    from_first = source == jnp.where(odd, 3 + 2 * axis, 2 + 2 * axis)
    from_second = source == jnp.where(odd, 2 + 2 * axis, 3 + 2 * axis)
    position = index & (count - 1)
    flip_first = (code & 1) == 1
    flip_second = (code & 2) == 2
    reverse = 7 - lax.broadcasted_iota(jnp.int32, (8, LANES), 0)

    def fetch(start):
        block, row = start // rows, start % rows
        one = lane_take(first_ref[row : row + 8], position + block * count)
        two = lane_take(second_ref[row : row + 8], position + (block ^ 1) * count)
        return jnp.where(from_first, one, jnp.where(from_second, two, local(start)))

    def turn(value):
        return jnp.take_along_axis(value, reverse, axis=0, mode="promise_in_bounds")

    def lines(p):
        q = NP - 1 - p
        pieces = [[fetch(line * NP), fetch(line * NP + 8)] for line in (p, q)]
        result = []
        for line, near, far in ((p, pieces[0], pieces[1]), (q, pieces[1], pieces[0])):
            first = [jnp.where(flip_first, far[h], near[h]) for h in range(2)]
            result.append((line, [jnp.where(flip_second, turn(first[1 - h]), first[h]) for h in range(2)]))
        return result

    return lines


def field_plane(field_ref, axis):
    def plane(side, start):
        layer = 1 if side == 0 else NP - 2
        if axis == 0:
            return field_ref[layer * PLANE + start : layer * PLANE + start + 8]
        if axis == 1:
            base = (start // NP) * PLANE + layer * NP + start % NP
            return field_ref[base : base + 8]
        return field_ref[pl.ds(start * NP + layer, 8, stride=NP)]

    return plane


def rim_plane(rim_ref, axis):
    def plane(side, start):
        base = (2 * axis + side) * PLANE + start
        return rim_ref[base : base + 8]

    return plane


def pack_kernel(field_ref, table_ref, o0, o1, o2, o3, o4, o5, ids_ref):
    outs = (o0, o1, o2, o3, o4, o5)
    start = 0
    for axis in range(3):
        count = LANES * outs[2 * axis].shape[0] // PLANE
        patterns = block_ids(table_ref[:, start : start + count], odd_place(axis))
        start += count
        for half in range(2):
            ids_ref[2 * axis + half : 2 * axis + half + 1] = patterns[half]
        pack_axis(axis, field_plane(field_ref, axis), patterns, count, outs[2 * axis], outs[2 * axis + 1])


def split(value):
    high = value.astype(BF16)
    return high, (value - high.astype(F32)).astype(BF16)


def stacked(value):
    high, low = split(value)
    return jnp.concatenate([high, high, low], axis=0)


def operator(value):
    high, low = split(value)
    return jnp.concatenate([high, low, high], axis=1)


def exact_dot(a, b):
    return jnp.dot(a, b, precision=lax.Precision.HIGHEST, preferred_element_type=F32)


def write_operators(s_ref, lam_ref, coeff_ref, main_ref, rim_ref, back_ref, to_ref, from_ref, base_ref, edge_ref):
    iota = lambda shape, dim: lax.broadcasted_iota(jnp.int32, shape, dim)

    def node(kidx, small_first):
        inner = kidx < PLANE
        t = kidx - PLANE
        group = t // NP
        along = 1 + t % NP
        if small_first:
            return jnp.where(inner, 1 + kidx // NP, jnp.where(group == 0, 0, jnp.where(group == 1, NE - 1, along)))
        return jnp.where(inner, 1 + kidx % NP, jnp.where(group == 2, 0, jnp.where(group == 3, NE - 1, along)))

    def hot(cond):
        return jnp.where(cond, 1.0, 0.0).astype(F32)

    wide_b = hot(iota((WIDE, NE), 0) // NE == iota((WIDE, NE), 1))
    wide_c = hot((iota((WIDE, NE), 0) % NE == iota((WIDE, NE), 1)) & (iota((WIDE, NE), 0) < NE * NE))
    wide_bt = hot(iota((NE, WIDE), 1) // NE == iota((NE, WIDE), 0))
    wide_ct = hot((iota((NE, WIDE), 1) % NE == iota((NE, WIDE), 0)) & (iota((NE, WIDE), 1) < NE * NE))
    node_j = hot(node(iota((NARROW, NE), 0), True) == iota((NARROW, NE), 1))
    node_k = hot(node(iota((NARROW, NE), 0), False) == iota((NARROW, NE), 1))
    node_jt = hot(node(iota((NE, NARROW), 1), True) == iota((NE, NARROW), 0))
    node_kt = hot(node(iota((NE, NARROW), 1), False) == iota((NE, NARROW), 0))
    s0, s1, s2 = s_ref[0], s_ref[1], s_ref[2]
    t0, t1, t2 = s0.T, s1.T, s2.T
    ahead = exact_dot(wide_b, exact_dot(t1, node_jt)) * exact_dot(wide_c, exact_dot(t2, node_kt))
    main_ref[...] = operator(ahead[:, :PLANE])
    rim_ref[...] = operator(ahead[:, PLANE:])
    back = exact_dot(node_j, exact_dot(s1, wide_bt)) * exact_dot(node_k, exact_dot(s2, wide_ct))
    back_ref[...] = operator(back)
    deep = hot(iota((DEEP, NE), 0) // CHUNK == iota((DEEP, NE), 1))
    deep_t = hot(iota((NE, DEEP), 1) // CHUNK == iota((NE, DEEP), 0))
    same = hot(iota((DEEP, DEEP), 0) % CHUNK == iota((DEEP, DEEP), 1) % CHUNK)
    to_ref[...] = operator(exact_dot(deep, exact_dot(t0, deep_t)) * same)
    from_ref[...] = operator(exact_dot(deep, exact_dot(s0, deep_t)) * same)
    col_b = jnp.sum(wide_b * lam_ref[1:2], axis=1, keepdims=True)
    col_c = jnp.sum(wide_c * lam_ref[2:3], axis=1, keepdims=True)
    base_ref[...] = col_b * coeff_ref[1:2] + col_c * coeff_ref[2:3]
    same_a = hot(iota((NE, NE), 0) == iota((NE, NE), 1))
    edge_ref[...] = jnp.sum(same_a * lam_ref[0:1], axis=1, keepdims=True) * coeff_ref[0:1]


def mm(a, b):
    return jnp.dot(a, b, preferred_element_type=F32)


def both(load):
    return jnp.concatenate([load(0), load(1)], axis=1)


def plane_rows(number, count=1):
    return slice(number * PLANE, (number + count) * PLANE)


def line_rows(face, line):
    return slice(face * PLANE + line * NP, face * PLANE + (line + 1) * NP)


def begin_kernel(
    field_ref, s_ref, lam_ref, coeff_ref, src_ref, idx_ref, code_ref,
    main_ref, rim_ref, back_ref, to_ref, from_ref, base_ref, edge_ref, table_ref, local_ref, work_ref,
):
    for n, ref in enumerate((src_ref, idx_ref, code_ref)):
        table_ref[n] = ref[...]
    write_operators(s_ref, lam_ref, coeff_ref, main_ref, rim_ref, back_ref, to_ref, from_ref, base_ref, edge_ref)
    for face in range(6):
        def put(start, value, face=face):
            local_ref[face * PLANE + start : face * PLANE + start + 8] = value

        local_face(
            face, field_plane(field_ref, face // 2), table_ref[0, face : face + 1], table_ref[1, face : face + 1], put
        )
    for pair in range(NP // 2):
        got = mm(main_ref[...], stacked(both(lambda s: field_ref[plane_rows(2 * pair + s)])))
        for s in range(2):
            work_ref[2 * pair + s] = got[:, s * LANES : (s + 1) * LANES]


def faces(local_ref, table_ref, messages):
    result = []
    for face in range(6):
        def local(start, face=face):
            return local_ref[face * PLANE + start : face * PLANE + start + 8]

        axis = face // 2
        rows = [table_ref[n, face : face + 1] for n in range(3)]
        result.append(unpack_face(face, local, odd_place(axis), messages[2 * axis], messages[2 * axis + 1], *rows))
    return result


def middle_kernel(
    local_ref, table_ref, ids_ref, first_ref, main_ref, rim_op_ref, back_ref, to_ref, from_ref, base_ref, edge_ref,
    m0, m1, m2, m3, m4, m5,
    work_ref, rim_ref, o0, o1, o2, o3, o4, o5,
    ghost_ref,
):
    outs = (o0, o1, o2, o3, o4, o5)
    for face, lines in enumerate(faces(local_ref, table_ref, (m0, m1, m2, m3, m4, m5))):
        for p in range(NP // 2):
            for line, pieces in lines(p):
                for h in range(2):
                    ghost_ref[pl.ds(face * PLANE + line * NP + 8 * h, 8)] = pieces[h]

    got = mm(main_ref[...], stacked(both(lambda s: ghost_ref[plane_rows(s)])))
    work_ref[0] = got[:, :LANES]
    work_ref[NE - 1] = got[:, LANES:]
    for pair in range(NP // 2):
        sides = [both(lambda s: ghost_ref[line_rows(f, 2 * pair + s)]) for f in range(2, 6)]
        got = mm(rim_op_ref[...], stacked(jnp.concatenate(sides, axis=0)))
        for s in range(2):
            i = 2 * pair + s
            work_ref[1 + i] = first_ref[i] + got[:, s * LANES : (s + 1) * LANES]

    for step in range(WIDE // CHUNK // 2):
        rows = [slice((2 * step + s) * CHUNK, (2 * step + s + 1) * CHUNK) for s in range(2)]
        chunk = both(lambda s: work_ref[:, rows[s], :].reshape(DEEP, LANES))
        coef = mm(to_ref[...], stacked(chunk))
        divisor = both(
            lambda s: jnp.concatenate([edge_ref[a : a + 1] + base_ref[rows[s], :] for a in range(NE)], axis=0)
        )
        solved = mm(from_ref[...], stacked(coef / divisor))
        for s in range(2):
            work_ref[:, rows[s], :] = solved[:, s * LANES : (s + 1) * LANES].reshape(NE, CHUNK, LANES)

    got = mm(back_ref[:PLANE], stacked(both(lambda s: work_ref[s * (NE - 1)])))
    rim_ref[plane_rows(0)] = got[:, :LANES]
    rim_ref[plane_rows(1)] = got[:, LANES:]
    for pair in range(NP // 2):
        got = mm(back_ref[PLANE:], stacked(both(lambda s: work_ref[1 + 2 * pair + s])))
        for s in range(2):
            for f in range(2, 6):
                rim_ref[line_rows(f, 2 * pair + s)] = got[(f - 2) * NP : (f - 1) * NP, s * LANES : (s + 1) * LANES]
    for axis in range(3):
        ids = [ids_ref[2 * axis + half : 2 * axis + half + 1] for half in range(2)]
        count = LANES * outs[2 * axis].shape[0] // PLANE
        pack_axis(axis, rim_plane(rim_ref, axis), ids, count, outs[2 * axis], outs[2 * axis + 1])


def inside_kernel(work_ref, back_ref, rim_ref, table_ref, inner_ref, local_ref):
    for pair in range(NP // 2):
        got = mm(back_ref[:PLANE], stacked(both(lambda s: work_ref[1 + 2 * pair + s])))
        for s in range(2):
            inner_ref[plane_rows(2 * pair + s)] = got[:, s * LANES : (s + 1) * LANES]
    for face in range(6):
        def put(start, value, face=face):
            local_ref[face * PLANE + start : face * PLANE + start + 8] = value

        local_face(face, rim_plane(rim_ref, face // 2), table_ref[0, face : face + 1], table_ref[1, face : face + 1], put)


def finish_kernel(inner_ref, local_ref, table_ref, m0, m1, m2, m3, m4, m5, out_hbm, out_ref, sems):
    sides = faces(local_ref, table_ref, (m0, m1, m2, m3, m4, m5))

    def add(place, value):
        out_ref[place] = out_ref[place] + value

    copies = []
    out_ref[plane_rows(1)] = inner_ref[plane_rows(1)]
    out_ref[plane_rows(NP - 2)] = inner_ref[plane_rows(NP - 2)]
    for face, layer in ((0, 1), (1, NP - 2)):
        for p in range(NP // 2):
            for line, pieces in sides[face](p):
                for h in range(2):
                    add(pl.ds(layer * PLANE + line * NP + 8 * h, 8), pieces[h])
    for p in range(NP // 2):
        for i in (p, NP - 1 - p):
            if i not in (1, NP - 2):
                out_ref[plane_rows(i)] = inner_ref[plane_rows(i)]
        for face in range(2, 6):
            layer = 1 if face % 2 == 0 else NP - 2
            for line, pieces in sides[face](p):
                for h in range(2):
                    if face < 4:
                        add(pl.ds(line * PLANE + layer * NP + 8 * h, 8), pieces[h])
                    else:
                        add(pl.ds((line * NP + 8 * h) * NP + layer, 8, stride=NP), pieces[h])
        for i in (p, NP - 1 - p):
            rows = plane_rows(i)
            copies.append(pltpu.make_async_copy(out_ref.at[rows], out_hbm.at[rows], sems.at[i]))
            copies[-1].start()
    for copy in copies:
        copy.wait()


VMEM = pl.BlockSpec(memory_space=pltpu.VMEM)
HBM = pl.BlockSpec(memory_space=pltpu.HBM)


def grant(mebibytes):
    return pltpu.CompilerParams(vmem_limit_bytes=mebibytes << 20)


def message_shapes(tables):
    shapes = []
    for table in tables:
        rows = PLANE * table.shape[1] // LANES
        shapes += [jax.ShapeDtypeStruct((rows, LANES), F32)] * 2
    return shapes


def exchange(messages, phase):
    arrived = [None] * 6
    for number in ORDERS[phase]:
        pairs = swap_pairs(number // 2, number % 2, lax.axis_size("dev"))
        arrived[number] = lax.ppermute(messages[number], "dev", pairs)
    return arrived


def shards(field, s_mats, lam, coeff, nbr_src, nbr_idx, orient, send_x, send_y, send_z):
    flat = field.reshape(NP * PLANE, LANES)
    tables = (send_x, send_y, send_z)
    shape = jax.ShapeDtypeStruct
    planes = shape((6 * PLANE, LANES), F32)
    block = shape((NP * PLANE, LANES), F32)
    packed = pl.pallas_call(
        pack_kernel, out_shape=message_shapes(tables) + [shape((8, LANES), jnp.int32)],
        in_specs=[VMEM] * 2, out_specs=[VMEM] * 7, compiler_params=grant(8), name="pack",
    )(flat, jnp.concatenate(tables, axis=1))
    outgoing, ids = packed[:6], packed[6]
    arrived = exchange(outgoing, 0)
    begun = pl.pallas_call(
        begin_kernel,
        out_shape=[
            shape((WIDE, 3 * PLANE), BF16), shape((WIDE, 12 * NP), BF16), shape((NARROW, 3 * WIDE), BF16),
            shape((DEEP, 3 * DEEP), BF16), shape((DEEP, 3 * DEEP), BF16), shape((WIDE, LANES), F32),
            shape((NE, LANES), F32), shape((3, 6, LANES), jnp.int32), planes, shape((NP, WIDE, LANES), F32),
        ],
        in_specs=[VMEM] * 7, out_specs=[VMEM] * 10,
        compiler_params=grant(20), name="begin",
        cost_estimate=pl.CostEstimate(flops=2 * 8 * WIDE * 1024 * 256, bytes_accessed=0, transcendentals=0),
    )(flat, s_mats, lam, coeff, nbr_src, nbr_idx, orient)
    operators, (table, local, first) = begun[:7], begun[7:]
    solved = pl.pallas_call(
        middle_kernel, out_shape=[shape((NE, WIDE, LANES), F32), planes] + message_shapes(tables),
        in_specs=[VMEM] * 17, out_specs=[VMEM] * 8, scratch_shapes=[pltpu.VMEM((6 * PLANE, LANES), F32)],
        compiler_params=grant(20), name="middle",
    )(local, table, ids, first, *operators, *arrived)
    work, rims = solved[:2]
    returned = exchange(solved[2:], 1)
    inner, local = pl.pallas_call(
        inside_kernel, out_shape=[block, planes], in_specs=[VMEM] * 4, out_specs=[VMEM] * 2,
        compiler_params=grant(16), name="inside",
        cost_estimate=pl.CostEstimate(flops=2 * 8 * PLANE * 1024 * 256, bytes_accessed=0, transcendentals=0),
    )(work, operators[2], rims, table)
    out = pl.pallas_call(
        finish_kernel, out_shape=block, in_specs=[VMEM] * 9, out_specs=HBM,
        scratch_shapes=[pltpu.VMEM(block.shape, F32), pltpu.SemaphoreType.DMA((NP,))],
        compiler_params=grant(12), name="finish",
    )(inner, local, table, *returned)
    return out.reshape(field.shape)


def solution(mesh):
    split_last = P(None, "dev")
    placed = (P(None, None, None, "dev"), P(), P()) + (split_last,) * 7
    return jax.shard_map(shards, mesh=mesh, in_specs=placed, out_specs=P(None, None, None, "dev"), check_vma=False)
```

```python
import jax
import jax.numpy as jnp
from jax import lax
from jax.experimental import pallas as pl
from jax.experimental.pallas import tpu as pltpu
from jax.sharding import PartitionSpec as P


DEV_X = 4
DEV_Y = 4
ORDERS = ((5, 4, 0, 1, 2, 3), (5, 4, 0, 1, 2, 3))
NP = 16
NE = 18
PLANE = NP * NP
LANES = 128
WIDE = 336
NARROW = PLANE + 4 * NP
CHUNK = 8
HALF = 4
STEPS = -(-NE * NE // CHUNK)
DEEP = 80
SIDE = 32
F32 = jnp.float32
BF16 = jnp.bfloat16


def swap_pairs(axis, turn, size):
    layout = (DEV_X, DEV_Y, size // (DEV_X * DEV_Y))
    stride = (1, DEV_X, DEV_X * DEV_Y)[axis]
    pairs = []
    for i in range(size):
        place = i // stride % layout[axis]
        other = place + 1 if place % 2 == turn else place - 1
        if 0 <= other < layout[axis]:
            pairs.append((i, i + (other - place) * stride))
        else:
            pairs.append((i, i ^ (DEV_X - 1 if axis == 0 else 1)))
    return pairs


def odd_place(axis):
    stride = (1, DEV_X, DEV_X * DEV_Y)[axis]
    return (lax.axis_index("dev") // stride) % 2 == 1


def lane_take(values, index):
    return jnp.take_along_axis(values, index, axis=1, mode="promise_in_bounds")


def lanes(shape):
    return lax.broadcasted_iota(jnp.int32, shape, 1)


def block_ids(table, odd):
    first = jnp.where(odd, table[0:1], table[1:2])
    second = jnp.where(odd, table[1:2], table[0:1])
    repeats = LANES // table.shape[1] // 2
    return [jnp.concatenate(pair * repeats, axis=1) for pair in ([first, second], [second, first])]


def pack_axis(axis, plane, ids, count, first_ref, second_ref):
    blocks = LANES // count
    rows = PLANE // blocks
    patterns = []
    for row in ids:
        row = jnp.broadcast_to(row, (8, LANES))
        patterns.append((row & (LANES - 1), (row // LANES) == 2 * axis + 1))
    lane_block = lanes((8, LANES)) // count
    for row in range(0, rows, 8):
        first_value = jnp.zeros((8, LANES), F32)
        second_value = jnp.zeros((8, LANES), F32)
        for block in range(blocks):
            slot, is_high = patterns[block % 2]
            start = block * rows + row
            got = jnp.where(is_high, lane_take(plane(1, start), slot), lane_take(plane(0, start), slot))
            first_value = jnp.where(lane_block == block, got, first_value)
            second_value = jnp.where(lane_block == block ^ 1, got, second_value)
        first_ref[row : row + 8] = first_value
        second_ref[row : row + 8] = second_value


def local_face(face, plane, source, index, put):
    axis = face // 2
    full = lambda row: jnp.broadcast_to(row, (8, LANES))
    source, index = full(source), full(index)
    slot = index & (LANES - 1)
    local = source == 1
    high = (index // LANES) == 2 * axis + 1
    for start in range(0, PLANE, 8):
        here = jnp.where(high, lane_take(plane(1, start), slot), lane_take(plane(0, start), slot))
        put(start, jnp.where(local, here, 0.0))


def unpack_face(face, local, odd, first_ref, second_ref, source, index, code):
    axis = face // 2
    rows = first_ref.shape[0]
    blocks = PLANE // rows
    count = LANES // blocks
    full = lambda row: jnp.broadcast_to(row, (8, LANES))
    source, index, code = full(source), full(index), full(code)
    from_first = source == jnp.where(odd, 3 + 2 * axis, 2 + 2 * axis)
    from_second = source == jnp.where(odd, 2 + 2 * axis, 3 + 2 * axis)
    position = index & (count - 1)
    flip_first = (code & 1) == 1
    flip_second = (code & 2) == 2
    reverse = 7 - lax.broadcasted_iota(jnp.int32, (8, LANES), 0)

    away = from_first | from_second
    odd_lane = (lanes((8, LANES)) // count) & 1 == 1
    places = [jnp.where(from_second, position + (block ^ 1) * count, position + block * count) for block in range(blocks)]

    def fetch(start):
        block, row = start // rows, start % rows
        one, two = first_ref[row : row + 8], second_ref[row : row + 8]
        mixed = jnp.where(odd_lane, one, two) if block % 2 else jnp.where(odd_lane, two, one)
        return jnp.where(away, lane_take(mixed, places[block]), local(start))

    def turn(value):
        return jnp.take_along_axis(value, reverse, axis=0, mode="promise_in_bounds")

    def lines(p):
        q = NP - 1 - p
        pieces = [[fetch(line * NP), fetch(line * NP + 8)] for line in (p, q)]
        result = []
        for line, near, far in ((p, pieces[0], pieces[1]), (q, pieces[1], pieces[0])):
            first = [jnp.where(flip_first, far[h], near[h]) for h in range(2)]
            result.append((line, [jnp.where(flip_second, turn(first[1 - h]), first[h]) for h in range(2)]))
        return result

    return lines


def field_plane(field_ref, axis):
    def plane(side, start):
        layer = 1 if side == 0 else NP - 2
        if axis == 0:
            return field_ref[layer * PLANE + start : layer * PLANE + start + 8]
        if axis == 1:
            base = (start // NP) * PLANE + layer * NP + start % NP
            return field_ref[base : base + 8]
        return field_ref[pl.ds(start * NP + layer, 8, stride=NP)]

    return plane


def rim_plane(rim_ref, axis):
    def plane(side, start):
        base = (2 * axis + side) * PLANE + start
        return rim_ref[base : base + 8]

    return plane


def pack_kernel(field_ref, table_ref, o0, o1, o2, o3, o4, o5, ids_ref, copy_ref):
    outs = (o0, o1, o2, o3, o4, o5)
    start = 0
    for axis in range(3):
        count = LANES * outs[2 * axis].shape[0] // PLANE
        patterns = block_ids(table_ref[0:2, start : start + count], odd_place(axis))
        start += count
        for half in range(2):
            ids_ref[2 * axis + half : 2 * axis + half + 1] = patterns[half]
        pack_axis(axis, field_plane(field_ref, axis), patterns, count, outs[2 * axis], outs[2 * axis + 1])
    copy_ref[...] = field_ref[...]


def split(value):
    high = value.astype(BF16)
    return high, (value - high.astype(F32)).astype(BF16)


def stacked(value):
    high, low = split(value)
    return jnp.concatenate([high, high, low], axis=0)


def operator(value):
    high, low = split(value)
    return jnp.concatenate([high, low, high], axis=1)


def parts(value):
    high = value.astype(BF16)
    rest = value - high.astype(F32)
    middle = rest.astype(BF16)
    return high, middle, (rest - middle.astype(F32)).astype(BF16)


def pick_columns(value, hot):
    return mm(jnp.concatenate(parts(value), axis=1), jnp.concatenate([hot] * 3, axis=0))


def pick_rows(hot, value):
    return mm(jnp.concatenate([hot] * 3, axis=1), jnp.concatenate(parts(value), axis=0))


def write_operators(s_ref, lam_ref, coeff_ref, main_ref, rim_ref, back_ref, to_ref, from_ref, ratio_ref, side_ref):
    iota = lambda shape, dim: lax.broadcasted_iota(jnp.int32, shape, dim)

    def node(kidx, small_first):
        block = kidx >> 4
        along = 1 + (kidx & (NP - 1))
        if small_first:
            rest = jnp.where(block == NP, 0, jnp.where(block == NP + 1, NE - 1, along))
            return jnp.where(block < NP, 1 + block, rest)
        return jnp.where(block == NP + 2, 0, jnp.where(block == NP + 3, NE - 1, along))

    def ones(cond):
        return jnp.where(cond, 1.0, 0.0).astype(F32)

    def hot(cond):
        return ones(cond).astype(BF16)

    def first_of(shape, dim):
        return (iota(shape, dim) * 3641) >> 16

    def second_of(shape, dim):
        number = iota(shape, dim)
        return jnp.where(number < NE * NE, number - NE * first_of(shape, dim), SIDE - 1)

    tall, flat = (WIDE, SIDE), (SIDE, WIDE)
    nodes, nodes_t = (NARROW, SIDE), (SIDE, NARROW)
    wide_b = hot(first_of(tall, 0) == iota(tall, 1))
    wide_c = hot(second_of(tall, 0) == iota(tall, 1))
    wide_bt = hot(first_of(flat, 1) == iota(flat, 0))
    wide_ct = hot(second_of(flat, 1) == iota(flat, 0))
    node_j = hot(node(iota(nodes, 0), True) == iota(nodes, 1))
    node_k = hot(node(iota(nodes, 0), False) == iota(nodes, 1))
    node_jt = hot(node(iota(nodes_t, 1), True) == iota(nodes_t, 0))
    node_kt = hot(node(iota(nodes_t, 1), False) == iota(nodes_t, 0))
    side_ref[...] = jnp.zeros(side_ref.shape, F32)
    side_ref[:, :NE, :NE] = s_ref[...]
    s0, s1, s2 = side_ref[0], side_ref[1], side_ref[2]
    t0, t1, t2 = s0.T, s1.T, s2.T
    ahead = pick_rows(wide_b, pick_columns(t1, node_jt)) * pick_rows(wide_c, pick_columns(t2, node_kt))
    main_ref[...] = operator(ahead[:, :PLANE])
    rim_ref[...] = operator(ahead[:, PLANE:])
    back = pick_rows(node_j, pick_columns(s1, wide_bt)) * pick_rows(node_k, pick_columns(s2, wide_ct))
    back_ref[...] = operator(back)
    deep = hot(iota((DEEP, SIDE), 0) >> 2 == iota((DEEP, SIDE), 1))
    deep_t = hot(iota((SIDE, DEEP), 1) >> 2 == iota((SIDE, DEEP), 0))
    same = ones((iota((DEEP, DEEP), 0) ^ iota((DEEP, DEEP), 1)) & (HALF - 1) == 0)
    to_ref[...] = operator(pick_rows(deep, pick_columns(t0, deep_t)) * same)
    from_ref[...] = operator(pick_rows(deep, pick_columns(s0, deep_t)) * same)
    side_ref[0, :3, :NE] = lam_ref[...]
    lam = [side_ref[0, n : n + 1] for n in range(3)]
    coeff = [coeff_ref[n : n + 1] for n in range(3)]

    def column(hots, row):
        return jnp.sum(hots.astype(F32) * row, axis=1, keepdims=True)

    base = column(wide_b, lam[1]) * coeff[1] + column(wide_c, lam[2]) * coeff[2]
    edge = column(deep, lam[0]) * coeff[0]
    upper = iota((CHUNK, LANES), 0) < HALF
    for step in range(STEPS):
        rows = base[step * CHUNK : (step + 1) * CHUNK]
        turned = pltpu.roll(rows, HALF, 0)
        ends = (jnp.where(upper, rows, turned), jnp.where(upper, turned, rows))
        for s in range(2):
            for m in range(NE // 2):
                ratio_ref[step, s, m] = 1.0 / (edge[m * CHUNK : (m + 1) * CHUNK] + ends[s])


def mm(a, b):
    return jnp.dot(a, b, preferred_element_type=F32)


def table_row(table_ref, number, face):
    row = 2 + 6 * number + face
    return table_ref[row : row + 1]


def both(load):
    return jnp.concatenate([load(0), load(1)], axis=1)


def plane_rows(number, count=1):
    return slice(number * PLANE, (number + count) * PLANE)


def line_rows(face, line):
    return slice(face * PLANE + line * NP, face * PLANE + (line + 1) * NP)


def begin_kernel(
    field_ref, table_ref, s_ref, lam_ref, coeff_ref,
    main_ref, rim_ref, back_ref, to_ref, from_ref, ratio_ref, local_ref, work_ref, side_ref,
):
    write_operators(s_ref, lam_ref, coeff_ref, main_ref, rim_ref, back_ref, to_ref, from_ref, ratio_ref, side_ref)
    for face in range(6):
        def put(start, value, face=face):
            local_ref[face * PLANE + start : face * PLANE + start + 8] = value

        local_face(
            face, field_plane(field_ref, face // 2), table_row(table_ref, 0, face), table_row(table_ref, 1, face), put
        )
    for pair in range(NP // 2):
        got = mm(main_ref[...], stacked(both(lambda s: field_ref[plane_rows(2 * pair + s)])))
        for s in range(2):
            work_ref[2 * pair + s] = got[:, s * LANES : (s + 1) * LANES]


def faces(local_ref, table_ref, messages):
    result = []
    for face in range(6):
        def local(start, face=face):
            return local_ref[face * PLANE + start : face * PLANE + start + 8]

        axis = face // 2
        rows = [table_row(table_ref, n, face) for n in range(3)]
        result.append(unpack_face(face, local, odd_place(axis), messages[2 * axis], messages[2 * axis + 1], *rows))
    return result


def middle_kernel(
    local_ref, table_ref, ids_ref, first_ref, main_ref, rim_op_ref, back_ref, to_ref, from_ref, ratio_ref,
    m0, m1, m2, m3, m4, m5,
    work_ref, rim_ref, o0, o1, o2, o3, o4, o5,
    ghost_ref,
):
    outs = (o0, o1, o2, o3, o4, o5)
    for face, lines in enumerate(faces(local_ref, table_ref, (m0, m1, m2, m3, m4, m5))):
        for p in range(NP // 2):
            for line, pieces in lines(p):
                for h in range(2):
                    ghost_ref[pl.ds(face * PLANE + line * NP + 8 * h, 8)] = pieces[h]

    got = mm(main_ref[...], stacked(both(lambda s: ghost_ref[plane_rows(s)])))
    work_ref[0] = got[:, :LANES]
    work_ref[NE - 1] = got[:, LANES:]
    for pair in range(NP // 2):
        sides = [both(lambda s: ghost_ref[line_rows(f, 2 * pair + s)]) for f in range(2, 6)]
        got = mm(rim_op_ref[...], stacked(jnp.concatenate(sides, axis=0)))
        for s in range(2):
            i = 2 * pair + s
            work_ref[1 + i] = first_ref[i] + got[:, s * LANES : (s + 1) * LANES]

    upper = lax.broadcasted_iota(jnp.int32, (CHUNK, LANES), 0) < HALF
    swap = lambda value: pltpu.roll(value, HALF, 0)
    spare = jnp.zeros((DEEP - NE * HALF, LANES), F32)
    pad = lambda pieces: jnp.concatenate(pieces + [spare], axis=0)
    for step in range(STEPS):
        rows = slice(step * CHUNK, (step + 1) * CHUNK)
        layers = [work_ref[i, rows, :] for i in range(NE)]
        pairs = list(zip(layers[0::2], layers[1::2]))
        left = pad([jnp.where(upper, a, swap(b)) for a, b in pairs])
        right = pad([jnp.where(upper, swap(a), b) for a, b in pairs])
        coef = mm(to_ref[...], stacked(jnp.concatenate([left, right], axis=1)))
        scaled = []
        for s in range(2):
            pieces = []
            for m in range(NE // 2):
                part = slice(m * CHUNK, (m + 1) * CHUNK)
                pieces.append(coef[part, s * LANES : (s + 1) * LANES] * ratio_ref[step, s, m])
            scaled.append(pad(pieces))
        solved = mm(from_ref[...], stacked(jnp.concatenate(scaled, axis=1)))
        for m in range(NE // 2):
            part = slice(m * CHUNK, (m + 1) * CHUNK)
            left, right = solved[part, :LANES], solved[part, LANES:]
            work_ref[2 * m, rows, :] = jnp.where(upper, left, swap(right))
            work_ref[2 * m + 1, rows, :] = jnp.where(upper, swap(left), right)

    got = mm(back_ref[:PLANE], stacked(both(lambda s: work_ref[s * (NE - 1)])))
    rim_ref[plane_rows(0)] = got[:, :LANES]
    rim_ref[plane_rows(1)] = got[:, LANES:]
    for pair in range(NP // 2):
        got = mm(back_ref[PLANE:], stacked(both(lambda s: work_ref[1 + 2 * pair + s])))
        for s in range(2):
            for f in range(2, 6):
                rim_ref[line_rows(f, 2 * pair + s)] = got[(f - 2) * NP : (f - 1) * NP, s * LANES : (s + 1) * LANES]
    for axis in range(3):
        ids = [ids_ref[2 * axis + half : 2 * axis + half + 1] for half in range(2)]
        count = LANES * outs[2 * axis].shape[0] // PLANE
        pack_axis(axis, rim_plane(rim_ref, axis), ids, count, outs[2 * axis], outs[2 * axis + 1])


def inside_kernel(work_ref, back_ref, rim_ref, table_ref, inner_ref, local_ref):
    for pair in range(NP // 2):
        got = mm(back_ref[:PLANE], stacked(both(lambda s: work_ref[1 + 2 * pair + s])))
        for s in range(2):
            inner_ref[plane_rows(2 * pair + s)] = got[:, s * LANES : (s + 1) * LANES]
    for face in range(6):
        def put(start, value, face=face):
            local_ref[face * PLANE + start : face * PLANE + start + 8] = value

        local_face(face, rim_plane(rim_ref, face // 2), table_row(table_ref, 0, face), table_row(table_ref, 1, face), put)


def finish_kernel(inner_ref, local_ref, table_ref, m0, m1, m2, m3, m4, m5, out_hbm, out_ref, sems):
    sides = faces(local_ref, table_ref, (m0, m1, m2, m3, m4, m5))

    def add(place, value):
        out_ref[place] = out_ref[place] + value

    copies = []
    out_ref[plane_rows(1)] = inner_ref[plane_rows(1)]
    out_ref[plane_rows(NP - 2)] = inner_ref[plane_rows(NP - 2)]
    for face, layer in ((0, 1), (1, NP - 2)):
        for p in range(NP // 2):
            for line, pieces in sides[face](p):
                for h in range(2):
                    add(pl.ds(layer * PLANE + line * NP + 8 * h, 8), pieces[h])
    for p in range(NP // 2):
        for i in (p, NP - 1 - p):
            if i not in (1, NP - 2):
                out_ref[plane_rows(i)] = inner_ref[plane_rows(i)]
        for face in range(2, 6):
            layer = 1 if face % 2 == 0 else NP - 2
            for line, pieces in sides[face](p):
                for h in range(2):
                    if face < 4:
                        add(pl.ds(line * PLANE + layer * NP + 8 * h, 8), pieces[h])
                    else:
                        add(pl.ds((line * NP + 8 * h) * NP + layer, 8, stride=NP), pieces[h])
        for i in (p, NP - 1 - p):
            rows = plane_rows(i)
            copies.append(pltpu.make_async_copy(out_ref.at[rows], out_hbm.at[rows], sems.at[i]))
            copies[-1].start()
    for copy in copies:
        copy.wait()


VMEM = pl.BlockSpec(memory_space=pltpu.VMEM)
HBM = pl.BlockSpec(memory_space=pltpu.HBM)


def grant(mebibytes):
    return pltpu.CompilerParams(vmem_limit_bytes=mebibytes << 20)


def message_shapes(tables):
    shapes = []
    for table in tables:
        rows = PLANE * table.shape[1] // LANES
        shapes += [jax.ShapeDtypeStruct((rows, LANES), F32)] * 2
    return shapes


def exchange(messages, phase):
    arrived = [None] * 6
    for number in ORDERS[phase]:
        pairs = swap_pairs(number // 2, number % 2, lax.axis_size("dev"))
        arrived[number] = lax.ppermute(messages[number], "dev", pairs)
    return arrived


def shards(field, s_mats, lam, coeff, nbr_src, nbr_idx, orient, send_x, send_y, send_z):
    flat = field.reshape(NP * PLANE, LANES)
    tables = (send_x, send_y, send_z)
    shape = jax.ShapeDtypeStruct
    planes = shape((6 * PLANE, LANES), F32)
    block = shape((NP * PLANE, LANES), F32)
    sends = jnp.concatenate([send_x, send_y, send_z, jnp.zeros((2, 32), jnp.int32)], axis=1)
    table = jnp.concatenate([sends, nbr_src, nbr_idx, orient], axis=0)
    packed = pl.pallas_call(
        pack_kernel, out_shape=message_shapes(tables) + [shape((8, LANES), jnp.int32), block],
        in_specs=[VMEM] * 2, out_specs=[VMEM] * 8, compiler_params=grant(8), name="pack",
    )(flat, table)
    outgoing, (ids, flat) = packed[:6], packed[6:]
    arrived = exchange(outgoing, 0)
    begun = pl.pallas_call(
        begin_kernel,
        out_shape=[
            shape((WIDE, 3 * PLANE), BF16), shape((WIDE, 12 * NP), BF16), shape((NARROW, 3 * WIDE), BF16),
            shape((DEEP, 3 * DEEP), BF16), shape((DEEP, 3 * DEEP), BF16),
            shape((STEPS, 2, NE // 2, CHUNK, LANES), F32), planes, shape((NP, WIDE, LANES), F32),
        ],
        in_specs=[VMEM] * 5, out_specs=[VMEM] * 8, scratch_shapes=[pltpu.VMEM((3, SIDE, SIDE), F32)],
        compiler_params=grant(20), name="begin",
        cost_estimate=pl.CostEstimate(flops=2 * 8 * WIDE * 1024 * 256, bytes_accessed=0, transcendentals=0),
    )(flat, table, s_mats, lam, coeff)
    operators, (local, first) = begun[:6], begun[6:]
    solved = pl.pallas_call(
        middle_kernel, out_shape=[shape((NE, WIDE, LANES), F32), planes] + message_shapes(tables),
        in_specs=[VMEM] * 16, out_specs=[VMEM] * 8, scratch_shapes=[pltpu.VMEM((6 * PLANE, LANES), F32)],
        compiler_params=grant(20), name="middle",
    )(local, table, ids, first, *operators, *arrived)
    work, rims = solved[:2]
    returned = exchange(solved[2:], 1)
    inner, local = pl.pallas_call(
        inside_kernel, out_shape=[block, planes], in_specs=[VMEM] * 4, out_specs=[VMEM] * 2,
        compiler_params=grant(16), name="inside",
        cost_estimate=pl.CostEstimate(flops=2 * 8 * PLANE * 1024 * 256, bytes_accessed=0, transcendentals=0),
    )(work, operators[2], rims, table)
    out = pl.pallas_call(
        finish_kernel, out_shape=block, in_specs=[VMEM] * 9, out_specs=HBM,
        scratch_shapes=[pltpu.VMEM(block.shape, F32), pltpu.SemaphoreType.DMA((NP,))],
        compiler_params=grant(12), name="finish",
    )(inner, local, table, *returned)
    return out.reshape(field.shape)


def solution(mesh):
    split_last = P(None, "dev")
    placed = (P(None, None, None, "dev"), P(), P()) + (split_last,) * 7
    return jax.shard_map(shards, mesh=mesh, in_specs=placed, out_specs=P(None, None, None, "dev"), check_vma=False)
```
